256 devices in a mesh: lon: 64 (over y, z, x_hi), lat: 4 (over x_lo, core).
Axes of the slice: x: 4 (x_hi: 2, x_lo: 2; x = x_hi * 2 + x_lo), y: 4, z: 8, core: 2. Of those that a mesh axis runs over, the one named last changes fastest.
Arguments:
- terrain_relief: float32 [1, 21504, 10752], P(None, 'lon', 'lat'), may hold values from -30 to 30
Outputs:
- smoothed: float32 [1, 21504, 10752], P(None, 'lon', 'lat')
- slope: float32 [1, 21504, 10752], P(None, 'lon', 'lat')
The draws below stay inside these ranges and needn't reach their ends.
All inputs are finite; a program needn't handle non-finite values.
Results may differ from the reference program's by a relative error of at most 0.0001.
Values sent between devices are 32-bit elements; how exact they have to be, the bound alone decides.
A program may use at most 64 MiB of HBM per device.

```python
import jax
import jax.numpy as jnp
from jax import lax

MEMBERS = 1
NLON = 21504
NLAT = 10752


def draw_terrain_relief(key, part):
    first_key, later_random_seed = jax.random.split(key, 2)
    grid_extent = (MEMBERS, NLON, NLAT)
    column = jnp.arange(NLON, dtype=jnp.float32)[None, :, None]
    trend = 1.0 + 2.0 * column / NLON
    factor = jnp.exp(jax.random.uniform(later_random_seed, grid_extent, jnp.float32, jnp.log(0.5), jnp.log(2.0)))
    noise = jnp.clip(jax.random.normal(first_key, grid_extent, jnp.float32), -4.0, 4.0)
    return (trend + 3.0 * factor * noise).astype(jnp.float32)


def setup_inputs(seed: int = 0) -> dict:
    keys = jax.random.split(jax.random.key(seed), 2)
    return {
        "terrain_relief": draw_terrain_relief(jax.random.fold_in(keys[1], 71), 0),
    }


def filter_pass(relief_surface):
    lat_count = relief_surface.shape[1]
    lon_sum = sum((jnp.roll(relief_surface, -offset, 0) for offset in range(-2, 3)))
    padded = jnp.pad(lon_sum, ((0, 0), (2, 2)))
    box_total = sum((padded[:, offset:offset + lat_count] for offset in range(5)))
    row_index = jnp.arange(lat_count, dtype=jnp.int32)
    counted = (jnp.minimum(row_index + 2, lat_count - 1) - jnp.maximum(row_index - 2, 0) + 1).astype(jnp.float32)
    final_output = box_total / (5.0 * counted)
    north_mean = jnp.mean(final_output[:, 0])
    south_mean = jnp.mean(final_output[:, lat_count - 1])
    final_output = final_output.at[:, 0].set(north_mean)
    final_output = final_output.at[:, lat_count - 1].set(south_mean)
    return final_output

def horn_slope(relief_surface):
    lat_count = relief_surface.shape[1]
    across = jnp.roll(relief_surface, -1, 0) - jnp.roll(relief_surface, 1, 0)
    padded_across = jnp.pad(across, ((0, 0), (1, 1)))
    east_west = padded_across[:, :-2] + 2.0 * padded_across[:, 1:-1] + padded_across[:, 2:]
    padded = jnp.pad(relief_surface, ((0, 0), (1, 1)))
    upward = padded[:, 2:] - padded[:, :-2]
    north_south = jnp.roll(upward, 1, 0) + 2.0 * upward + jnp.roll(upward, -1, 0)
    row_index = jnp.arange(lat_count, dtype=jnp.int32).astype(jnp.float32)
    latitude = jnp.pi * ((row_index + 0.5) / lat_count - 0.5)
    stretch = 1.0 / jnp.maximum(jnp.cos(latitude), 0.1)
    grad_x = east_west * stretch / 8.0
    grad_y = north_south / 8.0
    return jnp.sqrt(1.0 + grad_x * grad_x + grad_y * grad_y)

def sole_realization_case(relief_surface):
    for repetitions in range(2):
        relief_surface = filter_pass(relief_surface)
    return (relief_surface, horn_slope(relief_surface))

def reference(terrain_relief):
    return lax.map(sole_realization_case, terrain_relief)
```

```python
import functools
import math

import jax
import jax.numpy as jnp
import numpy as np
from jax import lax
from jax.experimental import pallas as pl
from jax.experimental.pallas import tpu as pltpu
from jax.sharding import PartitionSpec as P

MESH = pl.DeviceIdType.MESH
F32, BF16 = jnp.float32, jnp.bfloat16
LANES = 128
TILE = 8
ABOVE = 16
OVER = 24
DEPTH = 8
SCALE = 1.0 / 625.0


def stencils(smooth):
    ahead, behind = np.zeros_like(smooth), np.zeros_like(smooth)
    ahead[:, :-1], behind[:, 1:] = smooth[:, 1:], smooth[:, :-1]
    return np.concatenate([smooth, ahead + 2 * smooth + behind, ahead - behind], axis=1)


def five(width):
    at = np.arange(width)
    return (np.abs(at[:, None] - at[None, :]) <= 2).astype(np.float64)


def inner_weights():
    span = 4 * LANES
    parts = np.split(stencils(five(span) @ five(span)), 3, axis=1)
    return np.concatenate([p[:, LANES : 3 * LANES] for p in parts], axis=1)


def outer_weights(width, n_lat):
    total = width * n_lat
    lane = np.arange(LANES)
    out = []
    for band in range(n_lat):
        row = band * width + np.where(lane < 64, lane - TILE, width + lane - 120)
        near = (row == 1) | (row == total - 2)
        weight = np.where((row > 0) & (row < total - 1), np.where(near, 1 / 20, 1 / 25), 0.0)
        side = lane < 64
        box = five(LANES) * (side[:, None] == side[None, :])
        smooth = (box * weight[None, :]) @ (box * weight[None, :])
        ahead, behind = np.zeros_like(smooth), np.zeros_like(smooth)
        ahead[:, :-1], behind[:, 1:] = smooth[:, 1:], smooth[:, :-1]
        ahead[:, 63], behind[:, 64] = 0, 0
        out.append(np.concatenate([smooth, ahead + 2 * smooth + behind, ahead - behind], axis=1) / SCALE)
    return np.stack(out)


def column_sum(x, block, row):
    rows = [x[block, pl.ds(row + k, TILE), :] for k in range(-4, 5)]
    s = rows[4]
    value = s
    for k in range(1, 5):
        s = s + (rows[4 - k] + rows[4 + k])
        value = value + s
    return value * SCALE


def halves(value):
    high = value.astype(BF16)
    return high, (value - high.astype(F32)).astype(BF16)


def secant(east, before, middle, after):
    north = before + (middle + middle) + after
    square = 1.0 + east * east + (north * north) * (1.0 / 64.0)
    return square * lax.rsqrt(square)


def stretch_of(row, total):
    latitude = math.pi * ((row.astype(F32) + 0.5) / total - 0.5)
    return 0.125 / jnp.maximum(jnp.cos(latitude), 0.1)


def exchange(
    height, width, n_lon, n_lat, x, w_hbm, outer_high_hbm, outer_low_hbm, z, s,
    xb, vh, vl, q, d, ze, se, stretch, w, outer_high, outer_low, packed, landed, land_rows, corners,
    strip_high, strip_low, part, heard,
    block_sem, weight_sem, send, recv, polar_send, polar_recv,
):
    blocks = width // LANES
    tiles = height // TILE
    total = width * n_lat
    me, band = lax.axis_index("lon"), lax.axis_index("lat")
    up, down = lax.rem(me + 1, n_lon), lax.rem(me + n_lon - 1, n_lon)
    has_left, has_right = band > 0, band < n_lat - 1
    polar = (band == 0) | (band == n_lat - 1)

    depth = min(DEPTH, n_lon // 2)
    plane = n_lon // depth
    high = lax.rem(me, 2)
    deep = lax.rem(lax.div(me, 2), depth)
    broad = lax.div(me, 2 * depth)
    along, across = [], []
    for k in range(1, depth):
        along.append((broad * depth + lax.rem(deep + k, depth)) * 2 + high)
    for k in range(1, plane):
        other = lax.rem(broad * 2 + high + k, plane)
        across.append((lax.div(other, 2) * depth + deep) * 2 + lax.rem(other, 2))

    barrier = pltpu.get_barrier_semaphore()

    def greet(lon, lat):
        pl.semaphore_signal(barrier, inc=1, device_id=(lon, lat), device_id_type=MESH)

    for lon in (up, down):
        greet(lon, band)

    @pl.when(has_left)
    def _():
        for lon in (me, up, down):
            greet(lon, band - 1)

    @pl.when(has_right)
    def _():
        for lon in (me, up, down):
            greet(lon, band + 1)

    @pl.when(polar)
    def _():
        for lon in (*along, *across):
            greet(lon, band)

    def column(b):
        at = pl.ds(pl.multiple_of((b - 1) * LANES, LANES), LANES)
        return pltpu.make_async_copy(x.at[:, at], xb.at[b, pl.ds(OVER, height), :], block_sem.at[b - 1])

    for b in (1, blocks, *range(2, blocks)):
        column(b).start()
    weights = [
        pltpu.make_async_copy(w_hbm, w, weight_sem.at[0]),
        pltpu.make_async_copy(outer_high_hbm.at[band], outer_high, weight_sem.at[1]),
        pltpu.make_async_copy(outer_low_hbm.at[band], outer_low, weight_sem.at[2]),
    ]
    for copy in weights:
        copy.start()

    shape = stretch.shape
    tile_row = lax.broadcasted_iota(jnp.int32, shape, 0)
    tile_lane = lax.broadcasted_iota(jnp.int32, shape, 1)
    inside = (tile_row - 1) * LANES + tile_lane
    side_by_side = jnp.where(tile_lane < 64, tile_lane - TILE, width + tile_lane - 120)
    stretch[...] = stretch_of(band * width + jnp.where(tile_row == 0, side_by_side, inside), total)
    for b in (0, blocks + 1):
        for array in (vh, vl):
            array[:, LANES * b : LANES * b + LANES] = jnp.zeros((array.shape[0], LANES), BF16)
    for array in (strip_high, strip_low):
        array[0, :, 0:LANES] = jnp.zeros((32, LANES), BF16)
        array[blocks // 2, :, 3 * LANES : 4 * LANES] = jnp.zeros((32, LANES), BF16)

    lane = lax.broadcasted_iota(jnp.int32, (TILE, LANES), 1)
    group = lax.shift_right_logical(lane, 3)
    column(1).wait()
    column(blocks).wait()
    for side, b in ((0, 1), (1, blocks)):
        for first in range(0, tiles, 16):
            acc = jnp.zeros((TILE, LANES), F32)
            for t in range(first, min(first + 16, tiles)):
                k = t - first
                tile = xb[b, OVER + TILE * t : OVER + TILE * t + TILE, :]
                shift = (TILE * k + TILE * side) % LANES
                acc = jnp.where(group == k, pltpu.roll(tile, shift, 1) if shift else tile, acc)
            packed[side, first // 2 : first // 2 + TILE, :] = acc

    @pl.when(polar)
    def _():
        b = jnp.where(band == 0, 1, blocks)
        sums = [xb[b, OVER + TILE * t : OVER + TILE * t + TILE, :] for t in range(tiles)]
        while len(sums) > 1:
            sums = [p + r for p, r in zip(sums[::2], sums[1::2])] + ([sums[-1]] if len(sums) % 2 else [])
        part[0] = sums[0]

    def columns(b, carry):
        @pl.when((b > 1) & (b < blocks))
        def _():
            column(b).wait()

        at = pl.ds(pl.multiple_of(b * LANES, LANES), LANES)
        for t in range(height // 16):
            row = 16 * t
            value = jnp.concatenate([column_sum(xb, b, OVER + row + h) for h in (0, TILE)], axis=0)
            vh[ABOVE + row : ABOVE + row + 16, at], vl[ABOVE + row : ABOVE + row + 16, at] = halves(value)
        return carry

    def products(j, carry):
        b = jnp.minimum(1 + 2 * j, blocks - 1)
        window = pl.ds(pl.multiple_of((b - 1) * LANES, LANES), 4 * LANES)
        out = pl.ds(pl.multiple_of((b - 1) * LANES, LANES), 2 * LANES)
        own = pl.ds(ABOVE, height)
        first, second = vh[own, window], vl[own, window]
        for k in range(3):
            weight = w[:, 2 * LANES * k : 2 * LANES * (k + 1)]
            value = jnp.dot(first, weight, preferred_element_type=F32)
            value = value + jnp.dot(second, weight, preferred_element_type=F32)
            if k == 0:
                z[:, out] = value
            else:
                array = (q, d)[k - 1]
                array[b - 1, ABOVE : ABOVE + height, :] = value[:, :LANES]
                array[b, ABOVE : ABOVE + height, :] = value[:, LANES:]
        return carry

    def slopes(i, carry):
        row = pl.multiple_of(i * TILE, TILE)
        at = row + ABOVE
        for b in range(blocks):
            east = (q[b, pl.ds(at + 1, TILE), :] - q[b, pl.ds(at - 1, TILE), :]) * stretch[b + 1 : b + 2, :]
            rows = [d[b, pl.ds(at + k, TILE), :] for k in (-1, 0, 1)]
            s[pl.ds(row, TILE), LANES * b : LANES * b + LANES] = secant(east, *rows)
        return carry

    pairs = blocks // 2 + 1
    early = deep == 0
    columns_done = jnp.where(early, blocks, 0)
    pairs_done = jnp.where(early, pairs, 0)
    lax.fori_loop(1, 1 + columns_done, columns, 0)
    weights[0].wait()
    lax.fori_loop(0, pairs_done, products, 0)

    @pl.when(polar)
    def _():
        pl.semaphore_wait(barrier, 5 + len(along) + len(across))

    @pl.when(jnp.logical_not(polar))
    def _():
        pl.semaphore_wait(barrier, 8)

    def remote(src, dst, k, lon, lat):
        return pltpu.make_async_remote_copy(
            src, dst, send.at[k], recv.at[k], device_id=(lon, lat), device_id_type=MESH
        )

    head, tail = pl.ds(0, TILE), pl.ds(height - TILE, TILE)
    west, east = pl.ds(0, LANES), pl.ds(width - LANES, LANES)
    rows = [
        remote(x.at[tail, :], land_rows.at[0], 0, up, band),
        remote(x.at[head, :], land_rows.at[1], 1, down, band),
    ]
    to_left = [
        remote(packed.at[0], landed.at[1], 2, me, band - 1),
        remote(x.at[tail, west], corners.at[2], 3, up, band - 1),
        remote(x.at[head, west], corners.at[3], 4, down, band - 1),
    ]
    to_right = [
        remote(packed.at[1], landed.at[0], 5, me, band + 1),
        remote(x.at[tail, east], corners.at[0], 6, up, band + 1),
        remote(x.at[head, east], corners.at[1], 7, down, band + 1),
    ]

    def sums(stage, members, first):
        return [
            pltpu.make_async_remote_copy(
                part.at[stage], heard.at[first + k], polar_send.at[first + k], polar_recv.at[first + k],
                device_id=(lon, band), device_id_type=MESH,
            )
            for k, lon in enumerate(members)
        ]

    first_sums, second_sums = sums(0, along, 0), sums(1, across, len(along))

    @pl.when(polar)
    def _():
        for copy in first_sums:
            copy.start()

    for copy in rows:
        copy.start()

    @pl.when(has_left)
    def _():
        for copy in to_left:
            copy.start()

    @pl.when(has_right)
    def _():
        for copy in to_right:
            copy.start()

    lax.fori_loop(1 + columns_done, 1 + blocks, columns, 0)
    pairs_half = jnp.where(early, pairs, pairs // 2)
    lax.fori_loop(pairs_done, pairs_half, products, 0)

    @pl.when(polar)
    def _():
        for copy in first_sums:
            copy.wait_recv()
        value = part[0]
        for k in range(len(along)):
            value = value + heard[k]
        part[1] = value
        for copy in second_sums:
            copy.start()

    lax.fori_loop(pairs_half, pairs, products, 0)
    lax.fori_loop(0, tiles, slopes, 0)

    def pack(left, mine_left, mine_right, right, row):
        tile = jnp.where(
            lane < TILE, left, jnp.where(lane < 64, mine_left, jnp.where(lane < 120, mine_right, right))
        )
        xb[0, pl.ds(row, TILE), :] = tile

    def own_sides(row):
        return pltpu.roll(xb[1, pl.ds(row, TILE), :], TILE, 1), pltpu.roll(
            xb[blocks, pl.ds(row, TILE), :], LANES - TILE, 1
        )

    for t in range(tiles):
        row = OVER + TILE * t
        xb[0, row : row + TILE, :] = jnp.where(lane < 64, *own_sides(row))

    @pl.when(has_left)
    def _():
        for copy in to_right:
            copy.wait_recv()

    @pl.when(has_right)
    def _():
        for copy in to_left:
            copy.wait_recv()

    for copy in rows:
        copy.wait_recv()
    for end, row in ((0, OVER - TILE), (1, OVER + height)):
        for b in range(1, blocks + 1):
            xb[b, row : row + TILE, :] = land_rows[end, :, LANES * (b - 1) : LANES * b]
    for end, row in ((0, OVER - TILE), (1, OVER + height)):
        xb[0, row : row + TILE, :] = jnp.where(lane < 64, *own_sides(row))
    for side, there in ((0, has_left), (1, has_right)):
        mask = lane < TILE if side == 0 else lane >= LANES - TILE

        @pl.when(there)
        def _():
            for t in range(tiles):
                k = t % 16
                row = OVER + TILE * t
                tile = landed[side, t // 16 * TILE : t // 16 * TILE + TILE, :]
                shift = ((LANES - TILE * k) if side == 0 else (LANES - TILE - TILE * k)) % LANES
                tile = pltpu.roll(tile, shift, 1) if shift else tile
                xb[0, row : row + TILE, :] = jnp.where(mask, tile, xb[0, row : row + TILE, :])
            for end, row in ((0, OVER - TILE), (1, OVER + height)):
                shift = TILE if side == 0 else LANES - TILE
                tile = pltpu.roll(corners[2 * side + end], shift, 1)
                xb[0, row : row + TILE, :] = jnp.where(mask, tile, xb[0, row : row + TILE, :])

        @pl.when(jnp.logical_not(there))
        def _():
            for t in range(-1, tiles + 1):
                row = OVER + TILE * t
                xb[0, row : row + TILE, :] = jnp.where(mask, 0.0, xb[0, row : row + TILE, :])

    def strips(j, carry):
        for k in range(4):
            b = jnp.minimum(1 + 2 * j, blocks - 1) - 1 + k

            @pl.when((b > 0) & (b <= blocks))
            def _():
                for end, row in ((0, OVER - TILE), (1, OVER + height - TILE)):
                    value = jnp.concatenate([column_sum(xb, b, row + h) for h in (0, TILE)], axis=0)
                    at = slice(16 * end, 16 * end + 16)
                    cols = slice(LANES * k, LANES * k + LANES)
                    strip_high[j, at, cols], strip_low[j, at, cols] = halves(value)

        return carry

    lax.fori_loop(0, pairs, strips, 0)
    first = strip_high[...].reshape(pairs * 32, 4 * LANES)
    second = strip_low[...].reshape(pairs * 32, 4 * LANES)
    for k in range(3):
        weight = w[:, 2 * LANES * k : 2 * LANES * (k + 1)]
        value = jnp.dot(first, weight, preferred_element_type=F32)
        value = value + jnp.dot(second, weight, preferred_element_type=F32)
        for j in range(pairs):
            b = min(1 + 2 * j, blocks - 1)
            top, bottom = value[32 * j : 32 * j + 16], value[32 * j + 16 : 32 * j + 32]
            if k == 0:
                z[0:TILE, LANES * (b - 1) : LANES * (b + 1)] = top[TILE:]
                z[height - TILE : height, LANES * (b - 1) : LANES * (b + 1)] = bottom[:TILE]
            else:
                array = (q, d)[k - 1]
                for n in range(2):
                    cols = slice(LANES * n, LANES * n + LANES)
                    array[b - 1 + n, ABOVE - TILE : ABOVE + TILE, :] = top[:, cols]
                    array[b - 1 + n, ABOVE + height - TILE : ABOVE + height + TILE, :] = bottom[:, cols]
    slopes(0, 0)
    slopes(tiles - 1, 0)

    for copy in weights[1:]:
        copy.wait()
    for t in range(vh.shape[0] // 16):
        row = 16 * t
        value = jnp.concatenate([column_sum(xb, 0, OVER - ABOVE + row + h) for h in (0, TILE)], axis=0)
        vh[row : row + 16, 0:LANES], vl[row : row + 16, 0:LANES] = halves(value)
    first, second = vh[:, 0:LANES], vl[:, 0:LANES]
    value = jnp.dot(first, outer_high[...], preferred_element_type=F32)
    value = value + jnp.dot(second, outer_high[...], preferred_element_type=F32)
    value = value + jnp.dot(first, outer_low[...], preferred_element_type=F32)
    for k in range(3):
        ze[k] = value[:, LANES * k : LANES * k + LANES]

    @pl.when(polar)
    def _():
        for copy in second_sums:
            copy.wait_recv()
        value = part[1]
        for k in range(len(along), len(along) + len(across)):
            value = value + heard[k]
        north = band == 0
        away = jnp.where(north, lane, LANES - 1 - lane)
        one = 1.0 / (n_lon * height)
        first = jnp.sum(jnp.where(away < 3, value, 0.0)) * (one / 3.0)
        weights = jnp.where(
            away < 3, (1 / 3 + 1 / 4 + 1 / 5) / 3, jnp.where(away == 3, (1 / 4 + 1 / 5) / 3, 1 / 15)
        )
        second = jnp.sum(jnp.where(away < 5, value * weights, 0.0)) * one
        near, next_ = first * 0.25, first * 0.2
        away = jnp.where(north, lane - TILE, 119 - lane)
        lift = jnp.where(
            away == 0, second, jnp.where(away == 1, near, jnp.where(away == 2, next_, 0.0))
        )
        step = jnp.where(
            away == 0, near,
            jnp.where(
                away == 1, next_ - second,
                jnp.where(away == 2, -near, jnp.where(away == 3, -next_, 0.0)),
            ),
        )
        se[0] = lift
        se[1] = jnp.where(north, step, -step) * 4.0

    @pl.when(jnp.logical_not(polar))
    def _():
        se[0] = jnp.zeros((TILE, LANES), F32)
        se[1] = jnp.zeros((TILE, LANES), F32)

    lift, step = se[0], se[1]
    for t in range(tiles):
        row = TILE * t
        at = ABOVE + row
        east_ = (ze[1, at + 1 : at + 9, :] - ze[1, at - 1 : at + 7, :]) * stretch[0:1, :]
        before, middle, after = (ze[2, at + k : at + k + TILE, :] for k in (-1, 0, 1))
        slope = secant(east_, before + step, middle, after)
        smooth = ze[0, at : at + TILE, :] + lift
        here = slice(row, row + TILE)
        for array, value in ((z, smooth), (s, slope)):
            cols = slice(0, LANES)
            array[here, cols] = jnp.where(lane < TILE, pltpu.roll(value, LANES - TILE, 1), array[here, cols])
            cols = slice(width - LANES, width)
            array[here, cols] = jnp.where(lane < LANES - TILE, array[here, cols], pltpu.roll(value, TILE, 1))

    for copy in rows:
        copy.wait_send()

    @pl.when(has_left)
    def _():
        for copy in to_left:
            copy.wait_send()

    @pl.when(has_right)
    def _():
        for copy in to_right:
            copy.wait_send()

    @pl.when(polar)
    def _():
        for copy in (*first_sums, *second_sums):
            copy.wait_send()


def deliver(z, s, smoothed, slope, sems):
    parts = sems.shape[0] // 2
    span = z.shape[0] // parts
    copies = []
    for k in range(parts):
        at = pl.ds(k * span, span)
        copies.append(pltpu.make_async_copy(z.at[at, :], smoothed.at[at, :], sems.at[2 * k]))
        copies.append(pltpu.make_async_copy(s.at[at, :], slope.at[at, :], sems.at[2 * k + 1]))
    for copy in copies:
        copy.start()
    for copy in copies:
        copy.wait()


def local(n_lon, n_lat, terrain_relief):
    _, height, width = terrain_relief.shape
    blocks, tiles = width // LANES, height // TILE
    pairs = blocks // 2 + 1
    depth = min(DEPTH, n_lon // 2)
    others = depth + n_lon // depth - 2
    dma = pltpu.SemaphoreType.DMA
    outer = outer_weights(width, n_lat).astype(np.float32)
    outer_high = outer.astype(BF16)
    outer_low = (outer - outer_high.astype(np.float32)).astype(BF16)
    inner = inner_weights().astype(BF16)
    z, s = pl.pallas_call(
        functools.partial(exchange, height, width, n_lon, n_lat),
        out_shape=(pltpu.VMEM((height, width), F32), pltpu.VMEM((height, width), F32)),
        in_specs=[pl.BlockSpec(memory_space=pltpu.HBM)] * 4,
        out_specs=(pl.BlockSpec(memory_space=pltpu.VMEM), pl.BlockSpec(memory_space=pltpu.VMEM)),
        scratch_shapes=[
            pltpu.VMEM((blocks + 2, height + 2 * OVER, LANES), F32),
            pltpu.VMEM((height + 2 * ABOVE, width + 2 * LANES), BF16),
            pltpu.VMEM((height + 2 * ABOVE, width + 2 * LANES), BF16),
            pltpu.VMEM((blocks, height + 2 * ABOVE, LANES), F32),
            pltpu.VMEM((blocks, height + 2 * ABOVE, LANES), F32),
            pltpu.VMEM((3, height + 2 * ABOVE, LANES), F32),
            pltpu.VMEM((2, TILE, LANES), F32),
            pltpu.VMEM((-(-(blocks + 2) // TILE) * TILE, LANES), F32),
            pltpu.VMEM(inner.shape, BF16),
            pltpu.VMEM(outer.shape[1:], BF16),
            pltpu.VMEM(outer.shape[1:], BF16),
            pltpu.VMEM((2, -(-tiles // 16) * TILE, LANES), F32),
            pltpu.VMEM((2, -(-tiles // 16) * TILE, LANES), F32),
            pltpu.VMEM((2, TILE, width), F32),
            pltpu.VMEM((4, TILE, LANES), F32),
            pltpu.VMEM((pairs, 32, 4 * LANES), BF16),
            pltpu.VMEM((pairs, 32, 4 * LANES), BF16),
            pltpu.VMEM((2, TILE, LANES), F32),
            pltpu.VMEM((others, TILE, LANES), F32),
            dma((blocks,)),
            dma((3,)),
            dma((8,)),
            dma((8,)),
            dma((others,)),
            dma((others,)),
        ],
        compiler_params=pltpu.CompilerParams(
            collective_id=0, has_side_effects=True, vmem_limit_bytes=67043328 - 2 * 4 * height * width - 300000
        ),
    )(terrain_relief.reshape(height, width), jnp.asarray(inner), jnp.asarray(outer_high), jnp.asarray(outer_low))
    shape = jax.ShapeDtypeStruct((height, width), F32)
    smoothed, slope = pl.pallas_call(
        deliver,
        out_shape=(shape, shape),
        in_specs=[pl.BlockSpec(memory_space=pltpu.VMEM)] * 2,
        out_specs=(pl.BlockSpec(memory_space=pltpu.HBM),) * 2,
        scratch_shapes=[dma((12,))],
        compiler_params=pltpu.CompilerParams(vmem_limit_bytes=28 * 2**20),
    )(z, s)
    return smoothed.reshape(terrain_relief.shape), slope.reshape(terrain_relief.shape)


def solution(mesh):
    placed = P(None, "lon", "lat")
    return jax.shard_map(
        functools.partial(local, mesh.shape["lon"], mesh.shape["lat"]),
        mesh=mesh,
        in_specs=(placed,),
        out_specs=(placed, placed),
        check_vma=False,
    )
```
